32 devices in a mesh: lev: 2 (over x), w: 16 (over z, y, core).
Axes of the slice: x: 2, y: 2, z: 4, core: 2. Of those that a mesh axis runs over, the one named last changes fastest.
Arguments:
- coef: float32 [512, 2, 96, 512], P('w', None, 'lev'), parts along dimension 2
- legendre: float32 [512, 512, 512], replicated
- gauss_weight: float32 [512], replicated
Outputs:
- output 1: float32 [96, 512, 1024], P('lev', 'w'), parts along dimension 0
- output 2: float32 [512, 2, 96, 512], P('w', None, 'lev'), parts along dimension 2
There are 2 independent parts. The reference program is written for one: setup_inputs(seed, part) draws one part's arguments, and reference() takes and returns one part's arrays. A program takes and returns all parts, laid end to end along the dimension named above; an argument that names none is the same for every part.
All inputs are finite; a program needn't handle non-finite values.
Results may differ from the reference program's by a relative error of at most 0.001.
Values sent between devices are 32-bit elements.
A program may use at most 2.25 GiB of HBM per device.

```python
import jax
import jax.numpy as jnp
from jax import lax

WAVE_NUM = 512
LAT_ROWS = 512
LEVELS = 48


def setup_inputs(seed: int = 0, part: int = 0) -> dict:
    base_key = jax.random.key(seed)
    key_coef = jax.random.fold_in(jax.random.fold_in(base_key, 1), part)
    key_leg = jax.random.fold_in(base_key, 2)
    key_wt = jax.random.fold_in(base_key, 3)
    wave_idx = jnp.arange(WAVE_NUM)
    row_m = wave_idx[:, None].astype(jnp.float32)
    col_l = wave_idx[None, :].astype(jnp.float32)
    live_mask = wave_idx[None, :] >= wave_idx[:, None]
    amplitude = jnp.sqrt(WAVE_NUM / ((WAVE_NUM - row_m) * (1.0 + (col_l - row_m) / WAVE_NUM)))
    coef_mask = jnp.stack([live_mask, live_mask & (wave_idx[:, None] > 0)], axis=1)[:, :, None, :]
    draw_coef = jax.random.normal(key_coef, (WAVE_NUM, 2, LEVELS, WAVE_NUM), jnp.float32)
    coef = jnp.where(coef_mask, draw_coef * amplitude[:, None, None, :], 0.0)
    draw_leg = jax.random.normal(key_leg, (WAVE_NUM, WAVE_NUM, LAT_ROWS), jnp.float32)
    legendre = jnp.where(live_mask[:, :, None], draw_leg, 0.0)
    gauss_weight = jax.random.uniform(key_wt, (LAT_ROWS,), jnp.float32, 0.5, 1.5) / LAT_ROWS
    return {'coef': coef, 'legendre': legendre, 'gauss_weight': gauss_weight}


def reference(coef, legendre, gauss_weight):
    lon_pts = 2 * WAVE_NUM
    splits = 8
    lat_blk = LAT_ROWS // splits

    def lat_step(spec_acc, blk_idx):
        lat_start = blk_idx * lat_blk
        leg_blk = lax.dynamic_slice_in_dim(legendre, lat_start, lat_blk, axis=2).astype(jnp.float32)
        wt_blk = lax.dynamic_slice_in_dim(gauss_weight, lat_start, lat_blk, axis=0)
        fourier = jnp.einsum('mrkl,mlj->mrkj', coef.astype(jnp.float32), leg_blk)
        spec = lax.complex(fourier[:, 0], fourier[:, 1])
        grid_blk = jnp.fft.irfft(spec, n=lon_pts, axis=0)
        square_hat = jnp.fft.rfft(grid_blk * grid_blk, axis=0)[:WAVE_NUM] * wt_blk[None, None, :]
        re_im = jnp.stack([jnp.real(square_hat), jnp.imag(square_hat)], axis=1)
        spec_acc = spec_acc + jnp.einsum('mrkj,mlj->mrkl', re_im, leg_blk)
        return spec_acc, jnp.transpose(grid_blk, (1, 2, 0))

    spec_out, grid_parts = lax.scan(lat_step, jnp.zeros(coef.shape, jnp.float32), jnp.arange(splits))
    grid = jnp.transpose(grid_parts, (1, 0, 2, 3)).reshape(LEVELS, LAT_ROWS, lon_pts)
    return grid, spec_out
```

```python
import functools

import jax
import jax.numpy as jnp
import numpy as np
from jax import lax
from jax.experimental import pallas as pl
from jax.experimental.pallas import tpu as pltpu
from jax.sharding import PartitionSpec as P

F32, BF16 = jnp.float32, jnp.bfloat16
VMEM_LIMIT = 60 * 1024 * 1024
CHUNKS = (16, 16, 16)


def split_bf16(x):
    hi = x.astype(BF16)
    return hi, (x - hi.astype(F32)).astype(BF16)


def dot3(a, b, dims):
    d = functools.partial(lax.dot_general, dimension_numbers=(dims, ((), ())), preferred_element_type=F32)
    return d(a[0], b[0]) + d(a[1], b[0]) + d(a[0], b[1])


def swap_blocks(tiles, blk):
    lane = lax.broadcasted_iota(jnp.int32, (8, 128), 1)
    outs = []
    for s in range(4):
        acc = None
        for i in range(4):
            shift = (blk * (i - s)) % 128
            t = pltpu.roll(tiles[i], shift, 1) if shift else tiles[i]
            acc = t if acc is None else jnp.where(lane >= blk * i, t, acc)
        outs.append(acc)
    return outs


def dft_matrices(wave_num, group):
    wave_loc = wave_num // group
    par, owner, idx = np.meshgrid(np.arange(2), np.arange(group), np.arange(wave_loc // 2), indexing='ij')
    m = (owner * wave_loc + 2 * idx + par).reshape(2, -1)
    t = (m[:, :, None] * np.arange(wave_num)[None, None, :]) % (2 * wave_num)
    ang = 2.0 * np.pi * t / (2 * wave_num)
    full = np.concatenate([np.cos(ang), -np.sin(ang)], axis=1).astype(np.float32)
    hi = full.astype(jnp.bfloat16)
    lo = (full - hi.astype(np.float32)).astype(jnp.bfloat16)
    return np.stack([hi, lo])


def to_grid_kernel(levels, chunks, coef_ref, leg_ref, *refs):
    outs, held = refs[:-1], refs[-1]
    i = pl.program_id(0)
    rows = 2 * levels
    a = coef_ref[0].reshape(rows, coef_ref.shape[3])
    b = leg_ref[0]
    res = dot3(split_bf16(a), split_bf16(b), ((1,), (0,)))
    m_abs = lax.axis_index('w') * pl.num_programs(0) + i
    n_lon = 2.0 * leg_ref.shape[2]
    res = res * jnp.where(m_abs == 0, 1.0 / n_lon, 2.0 / n_lon)
    for z in range(4):
        held[z, pl.ds(pl.multiple_of((i % 16) * rows, 8), rows), :] = res[:, 128 * z:128 * z + 128]

    @pl.when(i % 16 == 15)
    def _():
        half = pl.multiple_of((i // 16) * 8, 8)

        def body(pr, _):
            par, r = pr // 2, pr % 2
            k0 = 0
            for out, kc in zip(outs, chunks):
                for kg in range(kc // 4):
                    for z in range(4):
                        start = par * rows + r * levels + k0 + 4 * kg
                        tiles = [held[z, pl.ds(start + k4, 8, stride=2 * rows), :] for k4 in range(4)]
                        for s, t in enumerate(swap_blocks(tiles, 32)):
                            out[4 * z + s, kg, par, r, pl.ds(half, 8), :] = t
                k0 += kc
            return 0

        lax.fori_loop(0, 4, body, 0)


def physics_kernel(f_ref, dft_ref, wt_ref, *refs):
    grid_ref, h_ref = refs[-2:]
    halves = []
    for par in range(2):
        x = jnp.concatenate(
            [jnp.concatenate([f_ref[:, kg, par, r].reshape(-1, 128) for r in range(2)], axis=0) for kg in range(2)], axis=1)
        xt = split_bf16(x.T)
        halves.append(dot3(xt, (dft_ref[0, par], dft_ref[1, par]), ((1,), (0,))))
    g1, g2 = halves[0] + halves[1], halves[0] - halves[1]
    n_half = g1.shape[1]
    grid_ref[:, :, :n_half] = g1.reshape(8, 32, n_half)
    grid_ref[:, :, n_half:] = g2.reshape(8, 32, n_half)
    q1, q2 = g1 * g1, g2 * g2
    for par in range(2):
        q = split_bf16(q1 + q2 if par == 0 else q1 - q2)
        h = dot3((dft_ref[0, par], dft_ref[1, par]), q, ((1,), (1,))) * wt_ref[...]
        half_rows = h.shape[0] // 2
        for kg in range(2):
            for r in range(2):
                h_ref[:, kg, par, r] = h[r * half_rows:(r + 1) * half_rows, 128 * kg:128 * kg + 128].reshape(-1, 16, 128)


def to_spec_kernel(chunks, leg_ref, *refs):
    n = len(chunks)
    ins, out_ref, held = refs[:n], refs[-2], refs[-1]
    i = pl.program_id(0)
    levels = sum(chunks)
    rows = 2 * levels

    @pl.when(i % 16 == 0)
    def _():
        half = pl.multiple_of((i // 16) * 8, 8)

        def body(pr, _):
            par, r = pr // 2, pr % 2
            k0 = 0
            for src, kc in zip(ins, chunks):
                for kg in range(kc // 4):
                    for z in range(4):
                        start = par * rows + r * levels + k0 + 4 * kg
                        tiles = [src[4 * z + s, kg, par, r, pl.ds(half, 8), :] for s in range(4)]
                        for k4, t in enumerate(swap_blocks(tiles, 32)):
                            held[z, pl.ds(start + k4, 8, stride=2 * rows), :] = t
                k0 += kc
            return 0

        lax.fori_loop(0, 4, body, 0)

    a = jnp.concatenate([held[z, pl.ds(pl.multiple_of((i % 16) * rows, 8), rows), :] for z in range(4)], axis=1)
    res = dot3(split_bf16(a), split_bf16(leg_ref[0]), ((1,), (1,)))
    out_ref[0] = res.reshape(2, levels, res.shape[1])


def solution(mesh):
    group = mesh.shape['w']

    def per_device(coef, legendre, gauss_weight):
        wave_loc, _, levels, n_deg = coef.shape
        lat_rows = legendre.shape[2]
        lat_loc = lat_rows // group
        wave_num = wave_loc * group
        dev = lax.axis_index('w')
        wt = lax.dynamic_slice_in_dim(gauss_weight, dev * lat_loc, lat_loc, axis=0)
        wt = jnp.tile(wt, 8)[None, :]
        dft = jnp.asarray(dft_matrices(wave_num, group))
        params = pltpu.CompilerParams(vmem_limit_bytes=VMEM_LIMIT)

        def f_shape(kc):
            return (group, kc // 4, 2, 2, 16, 128)

        leg_spec = pl.BlockSpec((1, n_deg, lat_rows), lambda i: (lax.axis_index('w') * wave_loc + i, 0, 0))
        fs = pl.pallas_call(
            functools.partial(to_grid_kernel, levels, CHUNKS),
            grid=(wave_loc,),
            out_shape=[jax.ShapeDtypeStruct(f_shape(kc), F32) for kc in CHUNKS],
            in_specs=[pl.BlockSpec((1, 2, levels, n_deg), lambda i: (i, 0, 0, 0)), leg_spec],
            out_specs=[pl.BlockSpec(f_shape(kc), lambda i: (0,) * 6) for kc in CHUNKS],
            scratch_shapes=[pltpu.VMEM((4, 16 * 2 * levels, 128), F32)],
            compiler_params=params,
            cost_estimate=pl.CostEstimate(flops=10 ** 10, bytes_accessed=50 * 10 ** 6, transcendentals=0),
            name='to_grid',
        )(coef, legendre)

        grid_out = None
        hs = []
        k0 = 0
        for f, kc in zip(fs, CHUNKS):
            f = lax.all_to_all(f, 'w', 0, 0, tiled=True)
            base = k0 // 8
            prev = [] if grid_out is None else [grid_out]
            fspec = pl.BlockSpec((group, 2, 2, 2, 16, 128), lambda i: (0, i, 0, 0, 0, 0))
            grid_out, h = pl.pallas_call(
                physics_kernel,
                grid=(kc // 8,),
                out_shape=[jax.ShapeDtypeStruct((levels, lat_loc, 2 * wave_num), F32), jax.ShapeDtypeStruct(f.shape, F32)],
                in_specs=[fspec, pl.BlockSpec(dft.shape, lambda i: (0, 0, 0, 0)), pl.BlockSpec(wt.shape, lambda i: (0, 0))]
                + [pl.BlockSpec(memory_space=pl.ANY)] * len(prev),
                out_specs=[pl.BlockSpec((8, lat_loc, 2 * wave_num), functools.partial(lambda b, i: (b + i, 0, 0), base)), fspec],
                input_output_aliases={3: 0} if prev else {},
                compiler_params=params,
                cost_estimate=pl.CostEstimate(flops=kc * 2 * 10 ** 8, bytes_accessed=kc * 4 * 10 ** 5, transcendentals=0),
                name='physics',
            )(f, dft, wt, *prev)
            hs.append(lax.all_to_all(h, 'w', 0, 0, tiled=True))
            k0 += kc

        spec = None
        k0 = 0
        for part in (tuple(range(len(CHUNKS) - 1)), (len(CHUNKS) - 1,)):
            kcs = tuple(CHUNKS[c] for c in part)
            tot = sum(kcs)
            prev = [] if spec is None else [spec]
            spec = pl.pallas_call(
                functools.partial(to_spec_kernel, kcs),
                grid=(wave_loc,),
                out_shape=jax.ShapeDtypeStruct(coef.shape, F32),
                in_specs=[leg_spec] + [pl.BlockSpec(f_shape(kc), lambda i: (0,) * 6) for kc in kcs]
                + [pl.BlockSpec(memory_space=pl.ANY)] * len(prev),
                out_specs=pl.BlockSpec((1, 2, tot, n_deg), functools.partial(lambda b, i: (i, 0, b, 0), k0 // tot)),
                scratch_shapes=[pltpu.VMEM((4, 16 * 2 * tot, 128), F32)],
                input_output_aliases={1 + len(kcs): 0} if prev else {},
                compiler_params=params,
                cost_estimate=pl.CostEstimate(flops=10 ** 10, bytes_accessed=50 * 10 ** 6, transcendentals=0),
                name='to_spec',
            )(legendre, *[hs[c] for c in part], *prev)
            k0 += tot
        return grid_out, spec

    return jax.shard_map(per_device, mesh=mesh, in_specs=(P('w', None, 'lev', None), P(None, None, None), P(None)), out_specs=(P('lev', 'w', None), P('w', None, 'lev', None)), check_vma=False)
```

```python
import functools

import jax
import jax.numpy as jnp
import numpy as np
from jax import lax
from jax.experimental import pallas as pl
from jax.experimental.pallas import tpu as pltpu
from jax.sharding import PartitionSpec as P

F32, BF16 = jnp.float32, jnp.bfloat16
VMEM_LIMIT = 63 * 1024 * 1024
RING = 4


def split_bf16(x):
    hi = x.astype(BF16)
    return hi, (x - hi.astype(F32)).astype(BF16)


def dot3(a, b, dims):
    d = functools.partial(lax.dot_general, dimension_numbers=(dims, ((), ())), preferred_element_type=F32)
    return d(a[0], b[0]) + d(a[1], b[0]) + d(a[0], b[1])


def swap_blocks(tiles, blk):
    lane = lax.broadcasted_iota(jnp.int32, (8, 128), 1)
    outs = []
    for s in range(4):
        acc = None
        for i in range(4):
            shift = (blk * (i - s)) % 128
            t = pltpu.roll(tiles[i], shift, 1) if shift else tiles[i]
            acc = t if acc is None else jnp.where(lane >= blk * i, t, acc)
        outs.append(acc)
    return outs


def dft_matrices(wave_num, group):
    wave_loc = wave_num // group
    par, owner, idx = np.meshgrid(np.arange(2), np.arange(group), np.arange(wave_loc // 2), indexing='ij')
    m = (owner * wave_loc + 2 * idx + par).reshape(2, -1)
    t = (m[:, :, None] * np.arange(wave_num)[None, None, :]) % (2 * wave_num)
    ang = 2.0 * np.pi * t / (2 * wave_num)
    full = np.concatenate([np.cos(ang), -np.sin(ang)], axis=1).astype(np.float32)
    hi = full.astype(jnp.bfloat16)
    lo = (full - hi.astype(np.float32)).astype(jnp.bfloat16)
    return np.stack([hi, lo])


def whole_kernel(group, coef, leg, dft_hbm, wt_ref, grid_out, spec_out,
                 f_send, x_recv, h_send, y_recv, held, leg_buf, coef_buf, dft, stage, spec_buf,
                 leg_sem, coef_sem, dft_sem, stage_sem, spec_sem, f_ssem, h_ssem, x_sem, y_sem):
    wave_loc, _, levels, n_deg = coef.shape
    rows = 2 * levels
    n_kg = levels // 4
    n_chunk = levels // 8
    lev, me = lax.axis_index('lev'), lax.axis_index('w')

    def peer(j):
        return lax.rem(me + j, group)

    barrier = pltpu.get_barrier_semaphore()

    def greet(j, _):
        pl.semaphore_signal(barrier, inc=1, device_id=(lev, peer(j)), device_id_type=pl.DeviceIdType.MESH)
        return 0

    lax.fori_loop(1, group, greet, 0)

    def wave_of(t):
        q, mm = t // 8, t % 8
        return 16 * (q // 2) + 2 * mm + q % 2

    def leg_copy(t):
        return pltpu.make_async_copy(leg.at[me * wave_loc + wave_of(t)], leg_buf.at[t % RING], leg_sem.at[t % RING])

    def coef_copy(t):
        return pltpu.make_async_copy(coef.at[wave_of(t)], coef_buf.at[t % RING], coef_sem.at[t % RING])

    def dft_copy():
        return pltpu.make_async_copy(dft_hbm, dft, dft_sem)

    def stage_copy(c):
        return pltpu.make_async_copy(stage.at[c % 2], grid_out.at[pl.ds(c * 8, 8)], stage_sem.at[c % 2])

    def spec_copy(t):
        return pltpu.make_async_copy(spec_buf.at[t % 2], spec_out.at[wave_of(t)], spec_sem.at[t % 2])

    def remote(src, dst, ssem, rsem, j):
        pltpu.make_async_remote_copy(src, dst, ssem, rsem, device_id=(lev, peer(j)), device_id_type=pl.DeviceIdType.MESH).start()

    for t in range(RING):
        leg_copy(t).start()
        coef_copy(t).start()
    dft_copy().start()

    for q in range(4):
        half, par = q // 2, q % 2

        def wave_in(mm, _):
            t = q * 8 + mm
            coef_copy(t).wait()
            leg_copy(t).wait()
            a = split_bf16(coef_buf[t % RING].reshape(rows, n_deg))
            res = dot3(a, split_bf16(leg_buf[t % RING]), ((1,), (0,)))
            m_abs = me * wave_loc + wave_of(t)
            n_lon = 2.0 * wave_loc * group
            res = res * jnp.where(m_abs == 0, 1.0 / n_lon, 2.0 / n_lon)
            for z in range(4):
                held[z, pl.ds(pl.multiple_of(mm * rows, 8), rows), :] = res[:, 128 * z:128 * z + 128]

            @pl.when(t + RING < wave_loc)
            def _():
                leg_copy(t + RING).start()
                coef_copy(t + RING).start()

            return 0

        lax.fori_loop(0, 8, wave_in, 0)

        def scatter(kr, _):
            kg, r = kr // 2, kr % 2
            for z in range(4):
                tiles = [held[z, pl.ds(r * levels + 4 * kg + k4, 8, stride=rows), :] for k4 in range(4)]
                for s, tile in enumerate(swap_blocks(tiles, 32)):
                    f_send[q, 4 * z + s, kg, r] = tile
            return 0

        lax.fori_loop(0, 2 * n_kg, scatter, 0)
        if q == 0:
            pl.semaphore_wait(barrier, group - 1)
        if q < 3:
            def send(j, _):
                remote(f_send.at[q, peer(j)], x_recv.at[:, par, :, me, half], f_ssem.at[q], x_sem.at[q], j)
                return 0

            lax.fori_loop(1, group, send, 0)
        else:
            def send(n, _):
                c, j = n // (group - 1), n % (group - 1) + 1
                remote(f_send.at[q, peer(j), pl.ds(2 * c, 2)], x_recv.at[pl.ds(2 * c, 2), par, :, me, half], f_ssem.at[q], x_sem.at[3 + c], j)
                return 0

            lax.fori_loop(0, n_chunk * (group - 1), send, 0)

        def keep(kg, _):
            x_recv[kg, par, :, me, half] = f_send[q, me, kg]
            return 0

        lax.fori_loop(0, n_kg, keep, 0)

    for t in range(RING):
        leg_copy(t).start()
    dft_copy().wait()
    for q in range(3):
        half, par = q // 2, q % 2
        blk = x_recv.at[:, par, :, pl.ds(0, group - 1), half]
        pltpu.make_async_copy(blk, blk, x_sem.at[q]).wait()

    def physics(c, _):
        blk = x_recv.at[pl.ds(2 * c, 2), 1, :, pl.ds(0, group - 1), 1]
        pltpu.make_async_copy(blk, blk, x_sem.at[3 + c]).wait()
        halves = []
        for par in range(2):
            x = jnp.concatenate(
                [jnp.concatenate([x_recv[2 * c + kg, par, r].reshape(-1, 128) for r in range(2)], axis=0) for kg in range(2)], axis=1)
            halves.append(dot3(split_bf16(x.T), (dft[0, par], dft[1, par]), ((1,), (0,))))
        g1, g2 = halves[0] + halves[1], halves[0] - halves[1]
        n_half = g1.shape[1]

        @pl.when(c >= 2)
        def _():
            stage_copy(c - 2).wait()

        stage[c % 2, :, :, :n_half] = g1.reshape(8, -1, n_half)
        stage[c % 2, :, :, n_half:] = g2.reshape(8, -1, n_half)
        stage_copy(c).start()
        q1, q2 = g1 * g1, g2 * g2
        for par in range(2):
            qs = split_bf16(q1 + q2 if par == 0 else q1 - q2)
            h = dot3((dft[0, par], dft[1, par]), qs, ((1,), (1,))) * wt_ref[...]
            half_rows = h.shape[0] // 2
            for kg in range(2):
                for r in range(2):
                    blk = h[r * half_rows:(r + 1) * half_rows, 128 * kg:128 * kg + 128].reshape(group, 2, 8, 128)
                    for half in range(2):
                        h_send[2 * half + par, :, 2 * c + kg, r] = blk[:, half]

        def send(n, _):
            q, j = n // (group - 1), n % (group - 1) + 1
            ks = pl.ds(2 * c, 2)
            remote(h_send.at[q, peer(j), ks], y_recv.at[q, me, ks], h_ssem.at[q], y_sem.at[q], j)
            return 0

        lax.fori_loop(0, 2 * (group - 1), send, 0)
        return 0

    lax.fori_loop(0, n_chunk, physics, 0)
    for q in range(2, 4):
        def send(j, _):
            remote(h_send.at[q, peer(j)], y_recv.at[q, me], h_ssem.at[q], y_sem.at[q], j)
            return 0

        lax.fori_loop(1, group, send, 0)

    for q in range(4):
        def keep(kg, _):
            y_recv[q, me, kg] = h_send[q, me, kg]
            return 0

        lax.fori_loop(0, n_kg, keep, 0)
        blk = y_recv.at[q, pl.ds(0, group - 1)]
        pltpu.make_async_copy(blk, blk, y_sem.at[q]).wait()

        def gather(kr, _):
            kg, r = kr // 2, kr % 2
            for z in range(4):
                tiles = [y_recv[q, 4 * z + s, kg, r] for s in range(4)]
                for k4, tile in enumerate(swap_blocks(tiles, 32)):
                    held[z, pl.ds(r * levels + 4 * kg + k4, 8, stride=rows), :] = tile
            return 0

        lax.fori_loop(0, 2 * n_kg, gather, 0)

        def wave_out(mm, _):
            t = q * 8 + mm
            a = jnp.concatenate([held[z, pl.ds(pl.multiple_of(mm * rows, 8), rows), :] for z in range(4)], axis=1)
            leg_copy(t).wait()
            res = dot3(split_bf16(a), split_bf16(leg_buf[t % RING]), ((1,), (1,)))

            @pl.when(t + RING < wave_loc)
            def _():
                leg_copy(t + RING).start()

            @pl.when(t >= 2)
            def _():
                spec_copy(t - 2).wait()

            spec_buf[t % 2] = res.reshape(2, levels, n_deg)
            spec_copy(t).start()
            return 0

        lax.fori_loop(0, 8, wave_out, 0)

    spec_copy(wave_loc - 2).wait()
    spec_copy(wave_loc - 1).wait()
    stage_copy(n_chunk - 2).wait()
    stage_copy(n_chunk - 1).wait()
    for q in range(4):
        blk = f_send.at[q, pl.ds(0, group - 1)]
        pltpu.make_async_copy(blk, blk, f_ssem.at[q]).wait()
        blk = h_send.at[q, pl.ds(0, group - 1)]
        pltpu.make_async_copy(blk, blk, h_ssem.at[q]).wait()


def solution(mesh):
    group = mesh.shape['w']

    def per_device(coef, legendre, gauss_weight):
        wave_loc, _, levels, n_deg = coef.shape
        lat_rows = legendre.shape[2]
        lat_loc = lat_rows // group
        wave_num = wave_loc * group
        n_kg = levels // 4
        dev = lax.axis_index('w')
        wt = lax.dynamic_slice_in_dim(gauss_weight, dev * lat_loc, lat_loc, axis=0)
        wt = jnp.tile(wt, 8)[None, :]
        dft = jnp.asarray(dft_matrices(wave_num, group))
        hbm = pl.BlockSpec(memory_space=pl.ANY)
        dma = pltpu.SemaphoreType.DMA
        return pl.pallas_call(
            functools.partial(whole_kernel, group),
            out_shape=[jax.ShapeDtypeStruct((levels, lat_loc, 2 * wave_num), F32), jax.ShapeDtypeStruct(coef.shape, F32)],
            in_specs=[hbm, hbm, hbm, pl.BlockSpec(memory_space=pltpu.VMEM)],
            out_specs=[hbm, hbm],
            scratch_shapes=[
                pltpu.VMEM((4, group, n_kg, 2, 8, 128), F32),
                pltpu.VMEM((n_kg, 2, 2, group, 2, 8, 128), F32),
                pltpu.VMEM((4, group, n_kg, 2, 8, 128), F32),
                pltpu.VMEM((4, group, n_kg, 2, 8, 128), F32),
                pltpu.VMEM((4, 8 * 2 * levels, 128), F32),
                pltpu.VMEM((RING, n_deg, lat_rows), F32),
                pltpu.VMEM((RING, 2, levels, n_deg), F32),
                pltpu.VMEM(dft.shape, BF16),
                pltpu.VMEM((2, 8, lat_loc, 2 * wave_num), F32),
                pltpu.VMEM((2, 2, levels, n_deg), F32),
                dma((RING,)), dma((RING,)), dma, dma((2,)), dma((2,)), dma((4,)), dma((4,)), dma((3 + levels // 8,)), dma((4,)),
            ],
            compiler_params=pltpu.CompilerParams(vmem_limit_bytes=VMEM_LIMIT, collective_id=0, has_side_effects=True),
            name='transform_pair',
        )(coef, legendre, dft, wt)

    return jax.shard_map(per_device, mesh=mesh, in_specs=(P('w', None, 'lev', None), P(None, None, None), P(None)), out_specs=(P('lev', 'w', None), P('w', None, 'lev', None)), check_vma=False)
```

```python
import functools

import jax
import jax.numpy as jnp
import numpy as np
from jax import lax
from jax.experimental import pallas as pl
from jax.experimental.pallas import tpu as pltpu
from jax.sharding import PartitionSpec as P

F32, BF16 = jnp.float32, jnp.bfloat16
VMEM_LIMIT = 50 * 1024 * 1024
RING = 4


def split_bf16(x):
    hi = x.astype(BF16)
    return hi, (x - hi.astype(F32)).astype(BF16)


def dot3(a, b, dims):
    d = functools.partial(lax.dot_general, dimension_numbers=(dims, ((), ())), preferred_element_type=F32)
    return d(a[0], b[0]) + d(a[1], b[0]) + d(a[0], b[1])


def swap_blocks(tiles, blk):
    lane = lax.broadcasted_iota(jnp.int32, (8, 128), 1)
    outs = []
    for s in range(4):
        acc = None
        for i in range(4):
            shift = (blk * (i - s)) % 128
            t = pltpu.roll(tiles[i], shift, 1) if shift else tiles[i]
            acc = t if acc is None else jnp.where(lane >= blk * i, t, acc)
        outs.append(acc)
    return outs


def dot3_stacked(a, b, dims):
    d = functools.partial(lax.dot_general, dimension_numbers=(dims, ((), ())), preferred_element_type=F32)
    n = a[0].shape[0]
    both = d(jnp.concatenate(a, axis=0), b[0])
    return both[:n] + both[n:] + d(a[0], b[1])


def dft_matrices(wave_num, group):
    wave_loc = wave_num // group
    par, owner, idx = np.meshgrid(np.arange(2), np.arange(group), np.arange(wave_loc // 2), indexing='ij')
    m = (owner * wave_loc + 2 * idx + par).reshape(2, -1)
    t = (m[:, :, None] * np.arange(wave_num)[None, None, :]) % (2 * wave_num)
    ang = 2.0 * np.pi * t / (2 * wave_num)
    full = np.concatenate([np.cos(ang), -np.sin(ang)], axis=1).astype(np.float32)
    hi = full.astype(jnp.bfloat16)
    lo = (full - hi.astype(np.float32)).astype(jnp.bfloat16)
    return np.stack([hi, lo])


def whole_kernel(group, coef, leg, dft_hbm, wt_ref, grid_out, spec_out,
                 f_send, x_recv, h_send, y_recv, held, leg_buf, coef_buf, dft,
                 leg_sem, coef_sem, dft_sem, f_ssem, h_ssem, x_sem, y_sem):
    wave_loc, _, levels, n_deg = coef.shape
    rows = 2 * levels
    n_kg = levels // 4
    n_chunk = levels // 8
    lev, me = lax.axis_index('lev'), lax.axis_index('w')

    def peer(j):
        return lax.rem(me + j, group)

    barrier = pltpu.get_barrier_semaphore()

    def greet(j, _):
        pl.semaphore_signal(barrier, inc=1, device_id=(lev, peer(j)), device_id_type=pl.DeviceIdType.MESH)
        return 0

    lax.fori_loop(1, group, greet, 0)

    def wave_of(t):
        q, mm = t // 8, t % 8
        return 16 * (q // 2) + 2 * mm + q % 2

    def leg_copy(t):
        return pltpu.make_async_copy(leg.at[me * wave_loc + wave_of(t)], leg_buf.at[t % RING], leg_sem.at[t % RING])

    def coef_copy(t):
        return pltpu.make_async_copy(coef.at[wave_of(t)], coef_buf.at[t % RING], coef_sem.at[t % RING])

    def dft_copy():
        return pltpu.make_async_copy(dft_hbm, dft, dft_sem)

    def remote(src, dst, ssem, rsem, j):
        pltpu.make_async_remote_copy(src, dst, ssem, rsem, device_id=(lev, peer(j)), device_id_type=pl.DeviceIdType.MESH).start()

    for t in range(RING):
        leg_copy(t).start()
        coef_copy(t).start()
    dft_copy().start()

    lane = lax.broadcasted_iota(jnp.int32, (1, 128), 1)
    wt = pltpu.roll(wt_ref[pl.ds(me // 4, 1), :], lax.rem(128 - 32 * lax.rem(me, 4), 128), 1)
    wt = jnp.where(lane < 32, wt, 0.0)
    wt = wt + pltpu.roll(wt, 32, 1)
    wt = wt + pltpu.roll(wt, 64, 1)
    wt = jnp.concatenate([wt, wt], axis=1)

    for q in range(4):
        half, par = q // 2, q % 2

        def wave_in(mm, _):
            t = q * 8 + mm
            coef_copy(t).wait()
            leg_copy(t).wait()
            a = split_bf16(coef_buf[t % RING].reshape(rows, n_deg))
            res = dot3_stacked(a, split_bf16(leg_buf[t % RING]), ((1,), (0,)))
            m_abs = me * wave_loc + wave_of(t)
            n_lon = 2.0 * wave_loc * group
            res = res * jnp.where(m_abs == 0, 1.0 / n_lon, 2.0 / n_lon)
            for z in range(4):
                held[z, pl.ds(pl.multiple_of(mm * rows, 8), rows), :] = res[:, 128 * z:128 * z + 128]

            @pl.when(t + RING < wave_loc)
            def _():
                leg_copy(t + RING).start()
                coef_copy(t + RING).start()

            return 0

        lax.fori_loop(0, 8, wave_in, 0)

        def scatter(kr, _):
            kg, r = kr // 2, kr % 2
            for z in range(4):
                tiles = [held[z, pl.ds(r * levels + 4 * kg + k4, 8, stride=rows), :] for k4 in range(4)]
                for s, tile in enumerate(swap_blocks(tiles, 32)):
                    f_send[q, 4 * z + s, kg, r] = tile
            return 0

        lax.fori_loop(0, 2 * n_kg, scatter, 0)
        if q == 0:
            pl.semaphore_wait(barrier, group - 1)
        if q < 3:
            def send(j, _):
                remote(f_send.at[q, peer(j)], x_recv.at[:, par, :, me, half], f_ssem.at[q], x_sem.at[q], j)
                return 0

            lax.fori_loop(1, group, send, 0)
        else:
            def send(n, _):
                c, j = n // (group - 1), n % (group - 1) + 1
                remote(f_send.at[q, peer(j), pl.ds(2 * c, 2)], x_recv.at[pl.ds(2 * c, 2), par, :, me, half], f_ssem.at[q], x_sem.at[3 + c], j)
                return 0

            lax.fori_loop(0, n_chunk * (group - 1), send, 0)

        def keep(kg, _):
            x_recv[kg, par, :, me, half] = f_send[q, me, kg]
            return 0

        lax.fori_loop(0, n_kg, keep, 0)

    for t in range(RING):
        leg_copy(t).start()
    dft_copy().wait()
    for q in range(3):
        half, par = q // 2, q % 2
        blk = x_recv.at[:, par, :, pl.ds(0, group - 1), half]
        pltpu.make_async_copy(blk, blk, x_sem.at[q]).wait()

    def physics(c, _):
        blk = x_recv.at[pl.ds(2 * c, 2), 1, :, pl.ds(0, group - 1), 1]
        pltpu.make_async_copy(blk, blk, x_sem.at[3 + c]).wait()
        halves = []
        for par in range(2):
            x = jnp.concatenate(
                [jnp.concatenate([x_recv[2 * c + kg, par, r].reshape(-1, 128) for r in range(2)], axis=0) for kg in range(2)], axis=1)
            halves.append(dot3(split_bf16(x.T), (dft[0, par], dft[1, par]), ((1,), (0,))))
        g1, g2 = halves[0] + halves[1], halves[0] - halves[1]
        n_half = g1.shape[1]

        grid_out[pl.ds(c * 8, 8), :, :n_half] = g1.reshape(8, -1, n_half)
        grid_out[pl.ds(c * 8, 8), :, n_half:] = g2.reshape(8, -1, n_half)
        q1, q2 = g1 * g1, g2 * g2
        for par in range(2):
            qs = split_bf16(q1 + q2 if par == 0 else q1 - q2)
            h = dot3((dft[0, par], dft[1, par]), qs, ((1,), (1,))) * wt
            half_rows = h.shape[0] // 2
            for kg in range(2):
                for r in range(2):
                    blk = h[r * half_rows:(r + 1) * half_rows, 128 * kg:128 * kg + 128].reshape(group, 2, 8, 128)
                    for half in range(2):
                        h_send[2 * half + par, :, 2 * c + kg, r] = blk[:, half]

        def send(n, _):
            q, j = n // (group - 1), n % (group - 1) + 1
            ks = pl.ds(2 * c, 2)
            remote(h_send.at[q, peer(j), ks], y_recv.at[q, me, ks], h_ssem.at[q], y_sem.at[q], j)
            return 0

        lax.fori_loop(0, 2 * (group - 1), send, 0)
        return 0

    lax.fori_loop(0, n_chunk, physics, 0)
    def send_h(q):
        def send(j, _):
            remote(h_send.at[q, peer(j)], y_recv.at[q, me], h_ssem.at[q], y_sem.at[q], j)
            return 0

        lax.fori_loop(1, group, send, 0)

    send_h(2)

    for q in range(4):
        def keep(kg, _):
            y_recv[q, me, kg] = h_send[q, me, kg]
            return 0

        lax.fori_loop(0, n_kg, keep, 0)
        blk = y_recv.at[q, pl.ds(0, group - 1)]
        pltpu.make_async_copy(blk, blk, y_sem.at[q]).wait()

        def gather(kr, _):
            kg, r = kr // 2, kr % 2
            for z in range(4):
                tiles = [y_recv[q, 4 * z + s, kg, r] for s in range(4)]
                for k4, tile in enumerate(swap_blocks(tiles, 32)):
                    held[z, pl.ds(r * levels + 4 * kg + k4, 8, stride=rows), :] = tile
            return 0

        lax.fori_loop(0, 2 * n_kg, gather, 0)

        def wave_out(mm, _):
            t = q * 8 + mm
            a = jnp.concatenate([held[z, pl.ds(pl.multiple_of(mm * rows, 8), rows), :] for z in range(4)], axis=1)
            leg_copy(t).wait()
            res = dot3_stacked(split_bf16(a), split_bf16(leg_buf[t % RING]), ((1,), (1,)))

            @pl.when(t + RING < wave_loc)
            def _():
                leg_copy(t + RING).start()

            spec_out[wave_of(t)] = res.reshape(2, levels, n_deg)
            return 0

        lax.fori_loop(0, 8, wave_out, 0)
        if q == 1:
            send_h(3)

    for q in range(4):
        blk = f_send.at[q, pl.ds(0, group - 1)]
        pltpu.make_async_copy(blk, blk, f_ssem.at[q]).wait()
        blk = h_send.at[q, pl.ds(0, group - 1)]
        pltpu.make_async_copy(blk, blk, h_ssem.at[q]).wait()


def solution(mesh):
    group = mesh.shape['w']

    def per_device(coef, legendre, gauss_weight):
        wave_loc, _, levels, n_deg = coef.shape
        lat_rows = legendre.shape[2]
        lat_loc = lat_rows // group
        wave_num = wave_loc * group
        n_kg = levels // 4
        wt = gauss_weight.reshape(4, 128)
        dft = jnp.asarray(dft_matrices(wave_num, group))
        hbm = pl.BlockSpec(memory_space=pl.ANY)
        dma = pltpu.SemaphoreType.DMA
        return pl.pallas_call(
            functools.partial(whole_kernel, group),
            out_shape=[pltpu.VMEM((levels, lat_loc, 2 * wave_num), F32), pltpu.VMEM(coef.shape, F32)],
            in_specs=[hbm, hbm, hbm, pl.BlockSpec(memory_space=pltpu.VMEM)],
            out_specs=[pl.BlockSpec(memory_space=pltpu.VMEM)] * 2,
            scratch_shapes=[
                pltpu.VMEM((4, group, n_kg, 2, 8, 128), F32),
                pltpu.VMEM((n_kg, 2, 2, group, 2, 8, 128), F32),
                pltpu.VMEM((4, group, n_kg, 2, 8, 128), F32),
                pltpu.VMEM((4, group, n_kg, 2, 8, 128), F32),
                pltpu.VMEM((4, 8 * 2 * levels, 128), F32),
                pltpu.VMEM((RING, n_deg, lat_rows), F32),
                pltpu.VMEM((RING, 2, levels, n_deg), F32),
                pltpu.VMEM(dft.shape, BF16),
                dma((RING,)), dma((RING,)), dma, dma((4,)), dma((4,)), dma((3 + levels // 8,)), dma((4,)),
            ],
            compiler_params=pltpu.CompilerParams(vmem_limit_bytes=VMEM_LIMIT, collective_id=0, has_side_effects=True),
            name='transform_pair',
        )(coef, legendre, dft, wt)

    return jax.shard_map(per_device, mesh=mesh, in_specs=(P('w', None, 'lev', None), P(None, None, None), P(None)), out_specs=(P('lev', 'w', None), P('w', None, 'lev', None)), check_vma=False)
```
